8 devices in a mesh: dp: 1 (over z), col: 2 (over y), row: 4 (over x, core).
Axes of the slice: x: 2, y: 2, z: 1, core: 2. Of those that a mesh axis runs over, the one named last changes fastest.
Arguments:
- act_in: bfloat16 [8192, 16384], P(('dp', 'row'), 'col')
- w_down: bfloat16 [16384, 4096], P('row', 'col')
- grad_out: bfloat16 [8192, 4096], P(('dp', 'row'), 'col')
Outputs:
- output 1: bfloat16 [8192, 16384], P(('dp', 'row'), 'col')
- output 2: float32 [16384, 4096], P(('dp', 'row'), 'col')
All inputs are finite; a program needn't handle non-finite values.
Results may differ from the reference program's by a relative error of at most 0.001.
Values are sent between devices in bfloat16 or wider.
A program may use at most 1 GiB of HBM per device.

```python
import jax
import jax.numpy as jnp

TOKENS = 8192
FEAT_IN = 16384
FEAT_OUT = 4096


def setup_inputs(seed: int = 0, part: int = 0) -> dict:
    base_key = jax.random.key(seed)
    key_w, key_part = jax.random.split(base_key)
    part_key = jax.random.fold_in(key_part, part)
    key_x, key_dy = jax.random.split(part_key)
    act_vals = jax.random.normal(key_x, (TOKENS, FEAT_IN), jnp.float32) * (TOKENS ** -0.5)
    weight_vals = jax.random.normal(key_w, (FEAT_IN, FEAT_OUT), jnp.float32) * (FEAT_OUT ** -0.5)
    grad_vals = jax.random.normal(key_dy, (TOKENS, FEAT_OUT), jnp.float32)
    return {"act_in": act_vals.astype(jnp.bfloat16), "w_down": weight_vals.astype(jnp.bfloat16), "grad_out": grad_vals.astype(jnp.bfloat16)}


def reference(act_in, w_down, grad_out):
    grad_in = jnp.dot(grad_out, w_down.T, preferred_element_type=jnp.float32).astype(jnp.bfloat16)
    grad_w = jnp.dot(act_in.T, grad_out, preferred_element_type=jnp.float32)
    return (grad_in, grad_w)
```

```python
import jax
import jax.numpy as jnp
from jax import lax
from jax.sharding import PartitionSpec as P


CHUNKS = 8
AHEAD = 6
AXES = ("col", "row")
W_ORDER = ("o0", "o1", "o2", "o3", "o4", "o5", "y0", "o6", "y1", "o7", "y2", "y3", "y4", "y5", "y6", "y7")


def _dev(x, y, q):
    return y * 4 + x * 2 + q


def _chips():
    return [(x, y, q) for x in (0, 1) for y in (0, 1) for q in (0, 1)]


Y_SWAP = [(_dev(x, y, q), _dev(x, 1 - y, q)) for x, y, q in _chips()]
X_SWAP = [(_dev(x, y, q), _dev(1 - x, y, q)) for x, y, q in _chips()]
X_CROSS = [(_dev(x, y, q), _dev(1 - x, y, q if x == y else 1 - q)) for x, y, q in _chips()]
Q_SWAP = [(_dev(x, y, q), _dev(x, y, 1 - q)) for x, y, q in _chips()]
Y_TO_DIAG = [pair for pair, (x, y, q) in zip(Y_SWAP, _chips()) if x != y]
Y_FROM_DIAG = [pair for pair, (x, y, q) in zip(Y_SWAP, _chips()) if x == y]


def _send(value, pairs):
    return lax.ppermute(value, AXES, pairs)


def _tie(value, *deps):
    deps = tuple(d for d in deps if d is not None)
    if not deps:
        return value
    return lax.optimization_barrier((value,) + deps)[0]


def _tdot(a, b):
    return lax.dot_general(a, b, (((0,), (0,)), ((), ())), preferred_element_type=jnp.float32)


def _dot(a, b):
    return lax.dot_general(a, b, (((1,), (0,)), ((), ())), preferred_element_type=jnp.float32)


def solution(mesh):
    io_spec = P(("dp", "row"), "col")
    w_spec = P("row", "col")

    def local_backward(act_blk, w_blk, grad_blk):
        row = lax.axis_index("row")
        col = lax.axis_index("col")
        core = row % 2
        diag = (row // 2) == col
        tokens, wide = act_blk.shape
        feats, outs = w_blk.shape
        half = outs // 2
        width = feats // CHUNKS

        def cut(a, j):
            return a[:, j * width : (j + 1) * width]

        g_y, g_x, g_d = [None] * 2, [None] * 2, [None] * 2
        piece = [grad_blk[:, :half], grad_blk[:, half:]]
        g_x[0] = _send(piece[0], X_SWAP)
        g_y[0] = _send(piece[0], Y_SWAP)
        g_d[0] = _send(g_x[0], Y_TO_DIAG)

        w_t = w_blk.T
        x_same = lax.dynamic_slice(act_blk, (0, core * feats), (tokens, feats))
        x_other = lax.dynamic_slice(act_blk, (0, (1 - core) * feats), (tokens, feats))

        g_q = _send(grad_blk, Q_SWAP)
        x_q = [_send(cut(x_other, j), Q_SWAP) for j in range(CHUNKS)]

        g_y[1] = _send(piece[1], Y_SWAP)

        g_x[1] = _send(piece[1], X_SWAP)
        g_d[1] = _send(g_x[1], Y_TO_DIAG)
        w_y = [_send(_tie(cut(w_t, j), g_d[0]), Y_TO_DIAG) for j in range(CHUNKS)]
        got, got_w = [], {}

        def exchange(p, dep=None):
            name = W_ORDER[p]
            j = int(name[1:])
            w_part = cut(w_t, j) if name[0] == "o" else w_y[j]
            x_part = cut(x_same if p % 2 == 0 else x_other, p // 2)
            if name[0] == "o":
                load = _tie(jnp.where(diag, w_part, x_part), dep)
            else:
                load = jnp.where(diag, w_part, _tie(x_part, dep))
            got.append(_send(load, X_SWAP if p % 2 == 0 else X_CROSS))
            got_w[name] = (w_part, got[-1], p)

        for p in range(AHEAD):
            exchange(p)

        g_yq = [_send(g, Q_SWAP) for g in g_y]
        g_xq = [_send(g, Q_SWAP) for g in g_x]
        g_dq = [_send(g, Q_SWAP) for g in g_d]
        g_yc = jnp.concatenate(g_y, axis=1)
        g_xc = jnp.concatenate(g_x, axis=1)
        g_xqc = jnp.concatenate(g_xq, axis=1)

        grad_in = jnp.zeros((tokens, wide), jnp.bfloat16)
        grad_w = jnp.zeros((feats, outs), jnp.float32)
        ready = {}
        last = None
        for step in range(CHUNKS):
            r1, r2 = got[2 * step], got[2 * step + 1]
            x_a, x_b = cut(x_same, step), x_q[step]
            r1, r2 = _tie(r1, last), _tie(r2, last)
            sent = []
            prev = None
            for h in range(2):
                local = _tdot(x_a, g_y[h]) + _tdot(x_b, g_yq[h])
                far = local + _tdot(_tie(r1, prev), g_d[h]) + _tdot(r2, g_dq[h])
                sent.append(_send(far, Y_FROM_DIAG))
                prev = far
            if step > 0:
                while len(got) < min(2 * step + AHEAD, 2 * CHUNKS):
                    exchange(len(got), prev)
            near = _tdot(x_a, grad_blk) + _tdot(x_b, g_q)
            near = near + _tdot(_tie(r1, prev), g_xc) + _tdot(r2, g_xqc)
            last = near
            for h in range(2):
                out = jnp.where(diag, near[:, h * half : (h + 1) * half], sent[h])
                grad_w = lax.dynamic_update_slice(grad_w, out, (step * width, h * half))
            for name, (w_part, recv, p) in list(got_w.items()):
                if p // 2 != step:
                    continue
                recv = _tie(recv, prev)
                mine = jnp.where(diag, _tie(w_part, recv), recv)
                ready[name] = (mine, _send(mine, Q_SWAP))
                if name[0] == "y":
                    j = int(name[1:])
                    for which, base in ((0, core * feats), (1, (1 - core) * feats)):
                        w_o = _tie(ready[f"o{j}"][which], prev)
                        w_n = ready[f"y{j}"][which]
                        part = (_dot(grad_blk, w_o) + _dot(g_yc, w_n)).astype(jnp.bfloat16)
                        grad_in = lax.dynamic_update_slice(grad_in, part, (0, base + j * width))
        return grad_in, grad_w

    return jax.shard_map(local_backward, mesh=mesh, in_specs=(io_spec, w_spec, io_spec), out_specs=(io_spec, io_spec), check_vma=False)
```

```python
import jax
import jax.numpy as jnp
from jax import lax
from jax.sharding import PartitionSpec as P


CHUNKS = 8
AHEAD = 5
AXES = ("col", "row")
W_ORDER = ("o0", "o1", "o2", "o3", "o4", "y0", "o5", "y1", "o6", "y2", "o7", "y3", "y4", "y5", "y6", "y7")


def _dev(x, y, q):
    return y * 4 + x * 2 + q


def _chips():
    return [(x, y, q) for x in (0, 1) for y in (0, 1) for q in (0, 1)]


Y_SWAP = [(_dev(x, y, q), _dev(x, 1 - y, q)) for x, y, q in _chips()]
X_SWAP = [(_dev(x, y, q), _dev(1 - x, y, q)) for x, y, q in _chips()]
X_CROSS = [(_dev(x, y, q), _dev(1 - x, y, q if x == y else 1 - q)) for x, y, q in _chips()]
Q_SWAP = [(_dev(x, y, q), _dev(x, y, 1 - q)) for x, y, q in _chips()]
Y_TO_DIAG = [pair for pair, (x, y, q) in zip(Y_SWAP, _chips()) if x != y]
Y_FROM_DIAG = [pair for pair, (x, y, q) in zip(Y_SWAP, _chips()) if x == y]


def _send(value, pairs):
    return lax.ppermute(value, AXES, pairs)


def _tie(value, *deps):
    deps = tuple(d for d in deps if d is not None)
    if not deps:
        return value
    return lax.optimization_barrier((value,) + deps)[0]


def _mm(a, b, over=0):
    return lax.dot_general(a, b, (((1,), (over,)), ((), ())), preferred_element_type=jnp.float32)


def solution(mesh):
    io_spec = P(("dp", "row"), "col")
    w_spec = P("row", "col")

    def local_backward(act_blk, w_blk, grad_blk):
        row = lax.axis_index("row")
        col = lax.axis_index("col")
        core = row % 2
        diag = (row // 2) == col
        tokens, wide = act_blk.shape
        feats, outs = w_blk.shape
        width = feats // CHUNKS

        def cut(a, j):
            return a[j * width : (j + 1) * width]

        g_x = _send(grad_blk, X_SWAP)
        g_y = _send(grad_blk, Y_SWAP)
        g_q = _send(grad_blk, Q_SWAP)

        x_same = lax.dynamic_slice(act_blk, (0, core * feats), (tokens, feats)).T
        x_other = lax.dynamic_slice(act_blk, (0, (1 - core) * feats), (tokens, feats)).T
        x_q = _send(x_other, Q_SWAP)
        near_own = _mm(x_same, grad_blk) + _mm(x_q, g_q)
        g_x, g_y = _tie(g_x, near_own), _tie(g_y, near_own)
        g_d = _send(g_x, Y_TO_DIAG)

        w_y = [_send(_tie(cut(w_blk, j), g_x), Y_TO_DIAG) for j in range(CHUNKS)]
        got, got_w = [], {}

        def exchange(p, dep=None):
            name = W_ORDER[p]
            j = int(name[1:])
            w_part = cut(w_blk, j) if name[0] == "o" else w_y[j]
            x_part = cut(x_same if p % 2 == 0 else x_other, p // 2)
            if name[0] == "o":
                load = _tie(jnp.where(diag, w_part, x_part), dep)
            else:
                load = jnp.where(diag, w_part, _tie(x_part, dep))
            got.append(_send(load, X_SWAP if p % 2 == 0 else X_CROSS))
            got_w[name] = (w_part, got[-1], p)

        for p in range(AHEAD):
            exchange(p)

        g_yq = _send(g_y, Q_SWAP)
        g_xx = jnp.concatenate([g_x, _send(g_x, Q_SWAP)], axis=0)
        far_own = _mm(x_same, g_y) + _mm(x_q, g_yq)
        g_all = jnp.concatenate([grad_blk, g_y], axis=1)
        g_d = _tie(g_d, far_own, g_xx, g_all)
        g_dd = jnp.concatenate([g_d, _send(g_d, Q_SWAP)], axis=0)

        def put(out, j, both):
            for w_full, base in zip(both, (core * feats, (1 - core) * feats)):
                part = _mm(g_all, w_full, over=1).astype(jnp.bfloat16)
                out = lax.dynamic_update_slice(out, part, (0, base + j * width))
            return out

        grad_in = jnp.zeros((tokens, wide), jnp.bfloat16)
        grad_w = jnp.zeros((feats, outs), jnp.float32)
        last, pending, landed = far_own, [], []

        def store(out, step, near, sent):
            return lax.dynamic_update_slice(out, jnp.where(diag, near, sent), (step * width, 0))

        for step in range(CHUNKS):
            grad_in, r1, r2, _ = lax.optimization_barrier((grad_in, got[2 * step], got[2 * step + 1], last))
            x_far = jnp.concatenate([r1, r2], axis=1)
            far = cut(far_own, step) + _mm(x_far, g_dd)
            sent = _send(far, Y_FROM_DIAG)
            while len(got) < min(2 * step + AHEAD + 1, 2 * CHUNKS):
                exchange(len(got), far)
            near = cut(near_own, step) + _mm(_tie(x_far, far), g_xx)
            last = near
            landed.append((step, near, sent))
            if step < CHUNKS - 3:
                grad_w = store(grad_w, *landed.pop(0))
            for j, both in pending:
                grad_in = put(grad_in, j, both)
            pending = []
            for name, (w_n, recv_n, p) in list(got_w.items()):
                if p // 2 != step or name[0] != "y":
                    continue
                j = int(name[1:])
                w_o, recv_o, _ = got_w[f"o{j}"]
                recv_o, recv_n = _tie(recv_o, far), _tie(recv_n, far)
                mine = jnp.concatenate(
                    [jnp.where(diag, _tie(w_o, recv_o), recv_o), jnp.where(diag, _tie(w_n, recv_n), recv_n)], axis=1
                )
                pending.append((j, (mine, _send(mine, Q_SWAP))))
        for j, both in pending:
            grad_in = put(grad_in, j, both)
        for step, near, sent in landed:
            grad_in, sent = lax.optimization_barrier((grad_in, sent))
            grad_w = store(grad_w, step, near, sent)
        return grad_in, grad_w

    return jax.shard_map(local_backward, mesh=mesh, in_specs=(io_spec, w_spec, io_spec), out_specs=(io_spec, io_spec), check_vma=False)
```

```python
import jax
import jax.numpy as jnp
from jax import lax
from jax.sharding import PartitionSpec as P


CHUNKS = 8
AHEAD = 5
AXES = ("col", "row")
W_ORDER = ("o0", "o1", "o2", "o3", "o4", "y0", "o5", "y1", "o6", "y2", "o7", "y3", "y4", "y5", "y6", "y7")


def _dev(x, y, q):
    return y * 4 + x * 2 + q


def _chips():
    return [(x, y, q) for x in (0, 1) for y in (0, 1) for q in (0, 1)]


Y_SWAP = [(_dev(x, y, q), _dev(x, 1 - y, q)) for x, y, q in _chips()]
X_SWAP = [(_dev(x, y, q), _dev(1 - x, y, q)) for x, y, q in _chips()]
X_CROSS = [(_dev(x, y, q), _dev(1 - x, y, q if x == y else 1 - q)) for x, y, q in _chips()]
Q_SWAP = [(_dev(x, y, q), _dev(x, y, 1 - q)) for x, y, q in _chips()]
Y_TO_DIAG = [pair for pair, (x, y, q) in zip(Y_SWAP, _chips()) if x != y]
Y_FROM_DIAG = [pair for pair, (x, y, q) in zip(Y_SWAP, _chips()) if x == y]


def _send(value, pairs):
    return lax.ppermute(value, AXES, pairs)


def _tie(value, *deps):
    deps = tuple(d for d in deps if d is not None)
    if not deps:
        return value
    return lax.optimization_barrier((value,) + deps)[0]


def _mm(a, b, over=0):
    return lax.dot_general(a, b, (((1,), (over,)), ((), ())), preferred_element_type=jnp.float32)


def solution(mesh):
    io_spec = P(("dp", "row"), "col")
    w_spec = P("row", "col")

    def local_backward(act_blk, w_blk, grad_blk):
        row = lax.axis_index("row")
        col = lax.axis_index("col")
        core = row % 2
        diag = (row // 2) == col
        tokens, wide = act_blk.shape
        feats, outs = w_blk.shape
        width = feats // CHUNKS

        def cut(a, j):
            return a[j * width : (j + 1) * width]

        g_x = _send(grad_blk, X_SWAP)
        g_y = _send(grad_blk, Y_SWAP)
        g_q = _send(grad_blk, Q_SWAP)

        x_same = lax.dynamic_slice(act_blk, (0, core * feats), (tokens, feats)).T
        x_other = lax.dynamic_slice(act_blk, (0, (1 - core) * feats), (tokens, feats)).T
        x_q = _send(x_other, Q_SWAP)
        near_own = _mm(x_same, grad_blk)
        g_x, g_y = _tie(g_x, near_own), _tie(g_y, near_own)
        near_own = near_own + _mm(x_q, g_q)
        g_d = _send(g_x, Y_TO_DIAG)

        w_y = [_send(_tie(cut(w_blk, j), g_x), Y_TO_DIAG) for j in range(CHUNKS)]
        got, got_w = [], {}

        def exchange(p, dep=None):
            name = W_ORDER[p]
            j = int(name[1:])
            w_part = cut(w_blk, j) if name[0] == "o" else w_y[j]
            x_part = cut(x_same if p % 2 == 0 else x_other, p // 2)
            if name[0] == "o":
                load = _tie(jnp.where(diag, w_part, x_part), dep)
            else:
                load = jnp.where(diag, w_part, _tie(x_part, dep))
            got.append(_send(load, X_SWAP if p % 2 == 0 else X_CROSS))
            got_w[name] = (w_part, got[-1], p)

        for p in range(AHEAD):
            exchange(p)

        g_yq = _send(g_y, Q_SWAP)
        g_xx = jnp.concatenate([g_x, _send(g_x, Q_SWAP)], axis=0)
        far_own = _mm(x_same, g_y) + _mm(x_q, g_yq)
        g_all = jnp.concatenate([grad_blk, g_y], axis=1)
        g_d = _tie(g_d, far_own, near_own, g_xx, g_all)
        g_dd = jnp.concatenate([g_d, _send(g_d, Q_SWAP)], axis=0)

        def put(out, j, both):
            for w_full, base in zip(both, (core * feats, (1 - core) * feats)):
                part = _mm(g_all, w_full, over=1).astype(jnp.bfloat16)
                out = lax.dynamic_update_slice(out, part, (0, base + j * width))
            return out

        grad_in = jnp.zeros((tokens, wide), jnp.bfloat16)
        grad_w = jnp.zeros((feats, outs), jnp.float32)
        last, pending, landed = far_own, [], []

        def store(out, step, near, sent):
            return lax.dynamic_update_slice(out, jnp.where(diag, near, sent), (step * width, 0))

        for step in range(CHUNKS):
            grad_in, r1, r2, _ = lax.optimization_barrier((grad_in, got[2 * step], got[2 * step + 1], last))
            x_far = jnp.concatenate([r1, r2], axis=1)
            far = cut(far_own, step) + _mm(x_far, g_dd)
            sent = _send(far, Y_FROM_DIAG)
            while len(got) < min(2 * step + AHEAD + 1, 2 * CHUNKS):
                exchange(len(got), far)
            near = cut(near_own, step) + _mm(_tie(x_far, far), g_xx)
            last = near
            landed.append((step, near, sent))
            if step < CHUNKS - 3:
                grad_w = store(grad_w, *landed.pop(0))
            for j, both in pending:
                grad_in = put(grad_in, j, both)
            pending = []
            for name, (w_n, recv_n, p) in list(got_w.items()):
                if p // 2 != step or name[0] != "y":
                    continue
                j = int(name[1:])
                w_o, recv_o, _ = got_w[f"o{j}"]
                recv_o, recv_n = _tie(recv_o, far), _tie(recv_n, far)
                mine = jnp.concatenate(
                    [jnp.where(diag, _tie(w_o, recv_o), recv_o), jnp.where(diag, _tie(w_n, recv_n), recv_n)], axis=1
                )
                pending.append((j, (mine, _send(mine, Q_SWAP))))
        for j, both in pending:
            grad_in = put(grad_in, j, both)
        for step, near, sent in landed:
            grad_in, sent = lax.optimization_barrier((grad_in, sent))
            grad_w = store(grad_w, step, near, sent)
        return grad_in, grad_w

    return jax.shard_map(local_backward, mesh=mesh, in_specs=(io_spec, w_spec, io_spec), out_specs=(io_spec, io_spec), check_vma=False)
```
